32 devices in a mesh: rows: 4 (over x, core), batch: 8 (over z, y).
Axes of the slice: x: 2, y: 2, z: 4, core: 2. Of those that a mesh axis runs over, the one named last changes fastest.
Arguments:
- features: bfloat16 [96, 8, 32, 512], P('batch', 'rows'), may hold values from -12 to 12
- norm_gain: float32 [512], replicated, may hold values from 0.25 to 1.75
- norm_bias: float32 [512], replicated, may hold values from -2.5 to 2.5
- conv_weight: bfloat16 [4, 4608], replicated, may hold values from -0.09375 to 0.09375
- embed_weight: float32 [16, 1024], replicated, may hold values from -1.5 to 1.5
- embed_bias: float32 [1024], replicated, may hold values from -2.5 to 2.5
- proj_in: bfloat16 [1024, 2048], P('rows'), may hold values from -0.1875 to 0.1875
- proj_in_bias: float32 [2048], replicated, may hold values from -2.5 to 2.5
- proj_out: bfloat16 [2048, 768], P('rows'), may hold values from -0.125 to 0.125
- proj_out_bias: float32 [768], replicated, may hold values from -2.5 to 2.5
- targets: bfloat16 [96, 4, 16, 768], P('batch', 'rows'), may hold values from -6 to 6
Outputs:
- grad_features: bfloat16 [96, 8, 32, 512], P('batch', 'rows')
- grad_conv: float32 [4, 4608], replicated
- grad_gain: float32 [512], replicated
- grad_bias: float32 [512], replicated
- grad_embed: float32 [16, 1024], replicated
The draws below stay inside these ranges and needn't reach their ends.
All inputs are finite; a program needn't handle non-finite values.
Results may differ from the reference program's by a relative error of at most 0.012.
Values may be sent and summed in bfloat16 or wider, within the bound.
A program may use at most 128 MiB of HBM per device.

```python
import jax
import jax.numpy as jnp
from jax import lax

CHANNELS = 512
GROUPS = 32
LATENT = 4
PATCH = 2
WIDTH = 1024
PROJ = 2048
ALIGN = 768
COLS = 32
IMAGES = 96
HEIGHT = 8
TOK_ROWS = 4
TOK_COLS = 16


def draw_features(key, part):
    key_base, key_chan = jax.random.split(key, 2)
    positions = jnp.arange(HEIGHT, dtype=jnp.float32)
    ramp = 1.0 + 2.0 * positions / max(HEIGHT - 1, 1)
    channel_scale = jnp.exp(jax.random.uniform(key_chan, (IMAGES, 1, 1, CHANNELS), minval=-0.7, maxval=0.7))
    base = jax.random.normal(key_base, (IMAGES, HEIGHT, COLS, CHANNELS))
    values = base * ramp[None, :, None, None] * channel_scale
    return jnp.clip(values, -12.0, 12.0).astype(jnp.bfloat16)


def block_levels(rng, shape, cuts, least, largest):
    def one(dim, shards_of):
        heights = jax.random.uniform(jax.random.fold_in(jax.random.fold_in(rng, 6), dim), (shards_of,), jnp.float32, least / len(cuts), largest / len(cuts))
        return jnp.repeat(jnp.exp(heights), shape[dim] // shards_of).reshape((-1,) + (1,) * (len(shape) - dim - 1))

    level = one(*cuts[0])
    for cut in cuts[1:]:
        level = level * one(*cut)
    return level


def noise(rng, dims, scale, most, cuts=(), kind=jnp.bfloat16):
    loudness = block_levels(rng, dims, cuts, -0.22, 0.18) if cuts else 1.0
    values = jax.random.normal(rng, dims, jnp.float32) * scale * loudness
    return jnp.minimum(jnp.maximum(values, -most), most).astype(kind)


def setup_inputs(seed: int = 0) -> dict:
    key_list = jax.random.split(jax.random.key(seed), 12)
    features = draw_features(jax.random.fold_in(key_list[11], 71), 0)
    norm_gain = jnp.clip(1.0 + 0.15 * jax.random.normal(key_list[1], (CHANNELS,), jnp.float32), 0.25, 1.75)
    norm_bias = noise(key_list[2], (CHANNELS,), 0.4, 2.5, (), jnp.float32)
    conv_weight = noise(key_list[3], (LATENT, 9 * CHANNELS), (9 * CHANNELS) ** -0.5, 0.09375)
    embed_weight = noise(key_list[4], (PATCH * PATCH * LATENT, WIDTH), (PATCH * PATCH * LATENT) ** -0.5, 1.5, (), jnp.float32)
    embed_bias = noise(key_list[5], (WIDTH,), 0.4, 2.5, (), jnp.float32)
    proj_in = noise(key_list[6], (WIDTH, PROJ), WIDTH ** -0.5, 0.1875, ((0, 4),))
    proj_in_bias = noise(key_list[7], (PROJ,), 0.4, 2.5, (), jnp.float32)
    proj_out = noise(key_list[8], (PROJ, ALIGN), PROJ ** -0.5, 0.125, ((0, 4),))
    proj_out_bias = noise(key_list[9], (ALIGN,), 0.4, 2.5, (), jnp.float32)
    targets = noise(key_list[10], (IMAGES, TOK_ROWS, TOK_COLS, ALIGN), 1.0, 6.0, ((0, 8), (1, 4)))
    return {"features": features, "norm_gain": norm_gain, "norm_bias": norm_bias, "conv_weight": conv_weight, "embed_weight": embed_weight, "embed_bias": embed_bias, "proj_in": proj_in, "proj_in_bias": proj_in_bias, "proj_out": proj_out, "proj_out_bias": proj_out_bias, "targets": targets}


EPS_NORM = 1e-06
EPS_UNIT = 1e-06

def swish_slope(values):
    sig = jax.nn.sigmoid(values)
    return sig * (1.0 + values * (1.0 - sig))

def one_image(feature_map, target_map, norm_gain, norm_bias, conv_weight, embed_weight, embed_bias, proj_in, proj_in_bias, proj_out, proj_out_bias):
    height, across, channels = feature_map.shape
    per_group = channels // GROUPS
    cell_count = height * across
    values = feature_map.astype(jnp.float32)
    grouped = values.reshape(cell_count, GROUPS, per_group)
    group_mean = lax.optimization_barrier(jnp.mean(grouped, axis=(0, 2), keepdims=True))
    centred = grouped - group_mean
    variance = lax.optimization_barrier(jnp.mean(centred * centred, axis=(0, 2), keepdims=True))
    inverse = lax.rsqrt(variance + EPS_NORM)
    normed = (centred * inverse).reshape(height, across, channels)
    shifted = normed * norm_gain + norm_bias
    active = (shifted * jax.nn.sigmoid(shifted)).astype(jnp.bfloat16)
    padded = jnp.pad(active, ((1, 1), (1, 1), (0, 0)))
    latent = jnp.zeros((cell_count, LATENT), jnp.float32)
    windows = []
    for position in range(9):
        row_off, col_off = (position // 3, position % 3)
        window = padded[row_off:row_off + height, col_off:col_off + across, :].reshape(cell_count, channels)
        windows.append(window)
        kernel = conv_weight[:, position * channels:(position + 1) * channels]
        latent = latent + lax.dot_general(window, kernel, (((1,), (1,)), ((), ())), preferred_element_type=jnp.float32)
    tok_rows = height // PATCH
    tok_cols = across // PATCH
    patches = latent.reshape(tok_rows, PATCH, tok_cols, PATCH, LATENT).transpose(0, 2, 1, 3, 4).reshape(tok_rows * tok_cols, PATCH * PATCH * LATENT)
    embedded = (jnp.dot(patches, embed_weight, precision=lax.Precision.HIGHEST) + embed_bias).astype(jnp.bfloat16)
    hidden_pre = jnp.dot(embedded, proj_in, preferred_element_type=jnp.float32) + proj_in_bias
    hidden_act = (hidden_pre * jax.nn.sigmoid(hidden_pre)).astype(jnp.bfloat16)
    projected = jnp.dot(hidden_act, proj_out, preferred_element_type=jnp.float32) + proj_out_bias
    target = target_map.reshape(tok_rows * tok_cols, -1).astype(jnp.float32)
    unit_target = target * lax.rsqrt(lax.optimization_barrier(jnp.sum(target * target, axis=1, keepdims=True)) + EPS_UNIT)
    inv_len = lax.rsqrt(lax.optimization_barrier(jnp.sum(projected * projected, axis=1, keepdims=True)) + EPS_UNIT)
    unit_proj = projected * inv_len
    cosine = lax.optimization_barrier(jnp.sum(unit_proj * unit_target, axis=1, keepdims=True))
    grad_out = (-inv_len * (unit_target - cosine * unit_proj)).astype(jnp.bfloat16)
    back_hidden = lax.dot_general(grad_out, proj_out, (((1,), (1,)), ((), ())), preferred_element_type=jnp.float32)
    grad_hidden = (back_hidden * swish_slope(hidden_pre)).astype(jnp.bfloat16)
    grad_embedded = lax.dot_general(grad_hidden, proj_in, (((1,), (1,)), ((), ())), preferred_element_type=jnp.float32)
    embed_part = lax.dot_general(patches, grad_embedded, (((0,), (0,)), ((), ())), precision=lax.Precision.HIGHEST)
    grad_patch = lax.dot_general(grad_embedded, embed_weight, (((1,), (1,)), ((), ())), precision=lax.Precision.HIGHEST)
    grad_latent = grad_patch.reshape(tok_rows, tok_cols, PATCH, PATCH, LATENT).transpose(0, 2, 1, 3, 4).reshape(height, across, LATENT).astype(jnp.bfloat16)
    grad_flat = grad_latent.reshape(cell_count, LATENT)
    grad_pad = jnp.pad(grad_latent, ((1, 1), (1, 1), (0, 0)))
    grad_active = jnp.zeros((cell_count, channels), jnp.float32)
    conv_parts = []
    for position in range(9):
        row_off, col_off = (position // 3, position % 3)
        conv_parts.append(lax.dot_general(grad_flat, windows[position], (((0,), (0,)), ((), ())), preferred_element_type=jnp.float32))
        back = grad_pad[2 - row_off:2 - row_off + height, 2 - col_off:2 - col_off + across, :].reshape(cell_count, LATENT)
        kernel = conv_weight[:, position * channels:(position + 1) * channels]
        grad_active = grad_active + jnp.dot(back, kernel, preferred_element_type=jnp.float32)
    conv_part = jnp.concatenate(conv_parts, axis=1)
    flat_shift = shifted.reshape(cell_count, channels)
    flat_normed = normed.reshape(cell_count, channels)
    grad_shift = grad_active * swish_slope(flat_shift)
    gain_part = lax.optimization_barrier(jnp.sum(grad_shift * flat_normed, axis=0))
    bias_part = lax.optimization_barrier(jnp.sum(grad_shift, axis=0))
    grad_norm = (grad_shift * norm_gain).reshape(cell_count, GROUPS, per_group)
    normed_groups = flat_normed.reshape(cell_count, GROUPS, per_group)
    first = lax.optimization_barrier(jnp.mean(grad_norm, axis=(0, 2), keepdims=True))
    second = lax.optimization_barrier(jnp.mean(grad_norm * normed_groups, axis=(0, 2), keepdims=True))
    grad_values = inverse * (grad_norm - first - normed_groups * second)
    grad_map = grad_values.reshape(height, across, channels).astype(jnp.bfloat16)
    return (grad_map, conv_part, gain_part, bias_part, embed_part)

def reference(features, norm_gain, norm_bias, conv_weight, embed_weight, embed_bias, proj_in, proj_in_bias, proj_out, proj_out_bias, targets):

    def step(pair):
        return one_image(pair[0], pair[1], norm_gain, norm_bias, conv_weight, embed_weight, embed_bias, proj_in, proj_in_bias, proj_out, proj_out_bias)
    grad_features, conv_parts, gain_parts, bias_parts, embed_parts = lax.map(step, (features, targets))
    return (grad_features, lax.optimization_barrier(jnp.sum(conv_parts, axis=0)), lax.optimization_barrier(jnp.sum(gain_parts, axis=0)), lax.optimization_barrier(jnp.sum(bias_parts, axis=0)), lax.optimization_barrier(jnp.sum(embed_parts, axis=0)))
```

```python
import functools

import jax
import jax.numpy as jnp
from jax import lax
from jax.experimental import pallas as pl
from jax.experimental.pallas import tpu as pltpu
from jax.sharding import PartitionSpec as P

GROUPS = 32
LATENT = 4
PATCH = 2
EPS_NORM = 1e-06
EPS_UNIT = 1e-06
F32 = jnp.float32
BF16 = jnp.bfloat16
NT = (((1,), (1,)), ((), ()))
TN = (((0,), (0,)), ((), ()))


def dot(a, b, dims=(((1,), (0,)), ((), ()))):
    return lax.dot_general(a, b, dims, preferred_element_type=F32)


def split(x, parts):
    out = []
    for _ in range(parts):
        part = x.astype(BF16).astype(F32)
        out.append(part)
        x = x - part
    return out


def exact_dot(x, exact, parts, dims=(((1,), (0,)), ((), ()))):
    rows = x.shape[0]
    full = dot(jnp.concatenate(split(x, parts), axis=0).astype(BF16), exact, dims)
    return sum(full[i * rows : (i + 1) * rows] for i in range(parts))


def kernel(
    images, height, across, n,
    feat, gain, bias, taps, wslice, win, winb, wout, woutb, targ,
    out, conv_o, gb_o, emb_o,
    st, st_in, nrm, slope, act, gs_ref, halo, halo_in, ghalo, ghalo_in,
    vpart, v_in, vcat, pout, hact, hslope, gh_ref, a_ref, a_in, fs, fs_in, stat,
    s_send, s_recv, v_send, v_recv, x_send, x_recv, b_send, b_recv,
    h_send, h_recv, g_send, g_recv, a_send, a_recv, f_send, f_recv,
):
    me = lax.axis_index("rows")
    cells, channels = feat.shape
    area = height * across
    per_group = channels // GROUPS
    members = n * area * per_group
    hidden = win.shape[1]
    share = wout.shape[0]
    tokens = targ.shape[0]
    tok_cols = across // PATCH
    prev, following = lax.rem(me + n - 1, n), lax.rem(me + 1, n)
    sibling = me + 1 - 2 * lax.rem(me, 2)

    def send(src, dst, ss, rs, peer):
        return pltpu.make_async_remote_copy(
            src_ref=src, dst_ref=dst, send_sem=ss, recv_sem=rs,
            device_id={"rows": peer}, device_id_type=pl.DeviceIdType.MESH,
        )

    def spread(src, dst, ss, rs):
        return [
            send(src, dst.at[k - 1], ss.at[k - 1], rs.at[k - 1], lax.rem(me + k, n))
            for k in range(1, n)
        ]

    barrier = pltpu.get_barrier_semaphore()
    for k in range(1, n):
        pl.semaphore_signal(
            barrier, inc=1, device_id={"rows": lax.rem(me + k, n)},
            device_id_type=pl.DeviceIdType.MESH,
        )
    pl.semaphore_wait(barrier, n - 1)

    def slab(owner):
        return pout.at[pl.ds(pl.multiple_of(owner * share, share), share), :]

    own = pl.ds(pl.multiple_of(me * share, share), share)
    cross = [
        send(wout, slab(me), x_send.at[k - 1], x_recv.at[k - 1], lax.rem(me + 2 * k, n))
        for k in range(1, n // 2)
    ]
    beside = [send(wout, slab(me), b_send.at[0], b_recv.at[0], sibling)]
    for copy in cross + beside:
        copy.start()
    pout[own, :] = wout[...]

    st[...] = jnp.zeros_like(st)

    def stats(b, carry):
        x = feat[pl.ds(pl.multiple_of(b * area, area), area), :].astype(F32)
        total = jnp.sum(x, axis=0, keepdims=True)
        centred = x - total / area
        st[0, pl.ds(b, 1), :] = total
        st[1, pl.ds(b, 1), :] = jnp.sum(centred * centred, axis=0, keepdims=True)
        return carry

    lax.fori_loop(0, images, stats, 0)
    stat_copies = spread(st, st_in, s_send, s_recv)
    for copy in stat_copies:
        copy.start()

    vpart[...] = exact_dot(wslice[...], win[...], 2)
    v_copies = spread(vpart, v_in, v_send, v_recv)
    for copy in v_copies:
        copy.start()
    same = (
        lax.broadcasted_iota(jnp.int32, (channels, channels), 0) // per_group
        == lax.broadcasted_iota(jnp.int32, (channels, channels), 1) // per_group
    )
    pool = jnp.where(same, 1.0, 0.0).astype(BF16)

    for copy in stat_copies:
        copy.wait()
    sums = [st[0]] + [st_in[k, 0] for k in range(n - 1)]
    squares = [st[1]] + [st_in[k, 1] for k in range(n - 1)]
    mean = exact_dot(sum(sums), pool, 3) / members
    spread_sq = sum(
        sq + area * jnp.square(total / area - mean) for total, sq in zip(sums, squares)
    )
    variance = exact_dot(spread_sq, pool, 3) / members
    stat[0] = mean
    stat[1] = lax.rsqrt(variance + EPS_NORM)

    def forward(b, carry):
        where = pl.ds(pl.multiple_of(b * area, area), area)
        x = feat[where, :].astype(F32)
        normed = (x - stat[0, pl.ds(b, 1), :]) * stat[1, pl.ds(b, 1), :]
        shifted = normed * gain[...] + bias[...]
        sig = jax.nn.sigmoid(shifted)
        nrm[where, :] = normed
        act[where, :] = (shifted * sig).astype(BF16)
        slope[where, :] = sig * (1.0 + shifted * (1.0 - sig))
        return carry

    lax.fori_loop(0, images, forward, 0)

    lane = lax.broadcasted_iota(jnp.int32, (8, cells), 1)
    col = lax.rem(lane, across)
    row = lax.rem(lane // across, height)

    def ahead(x, count):
        return pltpu.roll(x, (-count) % cells, 1) if count % cells else x

    def beside_col(x, off):
        if off == 0:
            return x
        ok = (col + off >= 0) & (col + off < across)
        return jnp.where(ok, ahead(x, off), 0.0)

    def above(x, arrived):
        edge = jnp.where(me > 0, ahead(arrived, (height - 1) * across), 0.0)
        return jnp.where(row == 0, edge, ahead(x, -across))

    def below(x, arrived):
        edge = jnp.where(me < n - 1, ahead(arrived, -(height - 1) * across), 0.0)
        return jnp.where(row == height - 1, edge, ahead(x, across))

    terms = dot(taps[...], act[...], NT)
    rows3 = []
    for dy in range(3):
        rows3.append(
            sum(
                beside_col(terms[(3 * dy + dx) * 8 : (3 * dy + dx + 1) * 8], dx - 1)
                for dx in range(3)
            )
        )
    halo[0] = rows3[0]
    halo[1] = rows3[2]
    halo_copies = [
        send(halo.at[0], halo_in.at[0], h_send.at[0], h_recv.at[0], following),
        send(halo.at[1], halo_in.at[1], h_send.at[1], h_recv.at[1], prev),
    ]
    for copy in halo_copies:
        copy.start()
    cell = lax.broadcasted_iota(jnp.int32, (cells, tokens), 0)
    tok = lax.broadcasted_iota(jnp.int32, (cells, tokens), 1)
    per_image = (height // PATCH) * tok_cols
    corner = (
        (tok // per_image) * area
        + (lax.rem(tok, per_image) // tok_cols) * (PATCH * across)
        + lax.rem(tok, tok_cols) * PATCH
    )
    away = cell - corner
    pick = [
        jnp.where(away == u * across + v, 1.0, 0.0).astype(BF16)
        for u in range(PATCH) for v in range(PATCH)
    ]
    for copy in v_copies:
        copy.wait()
    v_all = vpart[...] + sum(v_in[k] for k in range(n - 1))
    inner = PATCH * PATCH * LATENT
    v_hi, v_lo = split(v_all[0:inner], 2)
    vcat[...] = jnp.concatenate([v_hi, v_hi, v_lo], axis=0).astype(BF16)
    pre_bias = v_all[inner : inner + 1] + winb[...]
    for copy in halo_copies:
        copy.wait()
    latent = rows3[1] + above(rows3[0], halo_in[0]) + below(rows3[2], halo_in[1])
    first_half = lax.broadcasted_iota(jnp.int32, (8, tokens), 0) < LATENT
    blocks = []
    for u in range(PATCH):
        pair = [exact_dot(latent, pick[u * PATCH + v], 3) for v in range(PATCH)]
        blocks.append(jnp.where(first_half, pair[0], pair[1]))
    patches = jnp.concatenate(blocks, axis=0)
    p_hi, p_lo = split(patches, 2)
    pcat = jnp.concatenate([p_hi, p_lo, p_hi], axis=0).astype(BF16)

    for copy in cross:
        copy.wait()
    relay = []
    for k in range(1, n // 2):
        owner = lax.rem(me + n - 2 * k, n)
        relay.append(send(slab(owner), slab(owner), b_send.at[k], b_recv.at[k], sibling))
    for copy in relay:
        copy.start()

    step = hidden // 4
    for c in range(4):
        where = slice(c * step, (c + 1) * step)
        pre = dot(pcat, vcat[:, where], TN) + pre_bias[:, where]
        sig = jax.nn.sigmoid(pre)
        hact[:, where] = (pre * sig).astype(BF16)
        hslope[:, where] = sig * (1.0 + pre * (1.0 - sig))
    target = targ[...].astype(F32)
    unit_target = target * lax.rsqrt(jnp.sum(target * target, axis=1, keepdims=True) + EPS_UNIT)
    for copy in beside + relay:
        copy.wait()
    projected = dot(hact[...], pout[...]) + woutb[...]
    inv_len = lax.rsqrt(jnp.sum(projected * projected, axis=1, keepdims=True) + EPS_UNIT)
    unit_proj = projected * inv_len
    cosine = jnp.sum(unit_proj * unit_target, axis=1, keepdims=True)
    grad_out = (-inv_len * (unit_target - cosine * unit_proj)).astype(BF16)
    for c in range(4):
        where = slice(c * step, (c + 1) * step)
        back = dot(grad_out, pout[where, :], NT)
        gh_ref[:, where] = (back * hslope[:, where]).astype(BF16)
    two = dot(vcat[inner:, :], gh_ref[...], NT)
    grad_patch = (two[0:inner] + two[inner:]).astype(BF16)

    grid = []
    for v in range(PATCH):
        grid.append(
            sum(
                dot(grad_patch[u * 8 : (u + 1) * 8], pick[u * PATCH + v], NT)
                for u in range(PATCH)
            )
        )
    low_rows = lax.broadcasted_iota(jnp.int32, (8, cells), 0) < LATENT
    both = jnp.where(low_rows, grid[0], grid[1])
    grad_lat = both + pltpu.roll(both, LATENT, 0)
    grad_lat = jnp.where(low_rows, grad_lat, 0.0)
    ghalo[...] = grad_lat
    ghalo_copies = [
        send(ghalo, ghalo_in.at[0], g_send.at[0], g_recv.at[0], following),
        send(ghalo, ghalo_in.at[1], g_send.at[1], g_recv.at[1], prev),
    ]
    for copy in ghalo_copies:
        copy.start()
    wide = dot(pcat[0 : 2 * inner], gh_ref[...])
    a_ref[...] = wide[0:inner] + wide[inner:]
    a_copies = spread(a_ref, a_in, a_send, a_recv)
    for copy in a_copies:
        copy.start()
    for copy in ghalo_copies:
        copy.wait()
    by_row = [below(grad_lat, ghalo_in[1]), grad_lat, above(grad_lat, ghalo_in[0])]
    grad_taps = jnp.concatenate(
        [beside_col(by_row[dy], 1 - dx) for dy in range(3) for dx in range(3)], axis=0
    ).astype(BF16)
    gs_ref[...] = dot(grad_taps, taps[...], TN)
    fs[...] = jnp.zeros_like(fs)

    def backward(b, carry):
        where = pl.ds(pl.multiple_of(b * area, area), area)
        gs = gs_ref[where, :] * slope[where, :]
        gs_ref[where, :] = gs
        fs[0, pl.ds(b, 1), :] = jnp.sum(gs, axis=0, keepdims=True)
        fs[1, pl.ds(b, 1), :] = jnp.sum(gs * nrm[where, :], axis=0, keepdims=True)
        return carry

    lax.fori_loop(0, images, backward, 0)
    f_copies = spread(fs, fs_in, f_send, f_recv)
    for copy in f_copies:
        copy.start()
    gb_o[0:1, :] = jnp.sum(fs[1], axis=0, keepdims=True)
    gb_o[1:2, :] = jnp.sum(fs[0], axis=0, keepdims=True)
    gb_o[2:8, :] = jnp.zeros((6, channels), F32)
    conv_o[...] = dot(grad_taps, act[...])
    for copy in a_copies:
        copy.wait()
    a_all = a_ref[...] + sum(a_in[k] for k in range(n - 1))
    emb_o[...] = exact_dot(a_all, win[...], 2, NT)
    for copy in f_copies:
        copy.wait()
    for i in range(2):
        total = (fs[i] + sum(fs_in[k, i] for k in range(n - 1))) * gain[...]
        stat_i = exact_dot(total, pool, 3) / members
        stat[2 + i] = stat_i

    def finish(b, carry):
        where = pl.ds(pl.multiple_of(b * area, area), area)
        one = pl.ds(b, 1)
        out[where, :] = (
            stat[1, one, :]
            * (gs_ref[where, :] * gain[...] - stat[2, one, :] - nrm[where, :] * stat[3, one, :])
        ).astype(BF16)
        return carry

    lax.fori_loop(0, images, finish, 0)


def shards(
    features, norm_gain, norm_bias, conv_weight, embed_weight, embed_bias,
    proj_in, proj_in_bias, proj_out, proj_out_bias, targets,
):
    images, height, across, channels = features.shape
    n = lax.axis_size("rows")
    me = lax.axis_index("rows")
    cells = images * height * across
    align = targets.shape[-1]
    tokens = targets.shape[0] * targets.shape[1] * targets.shape[2]
    inner, width = embed_weight.shape
    part, hidden = proj_in.shape
    share = proj_out.shape[0]
    pad_images = -(-images // 8) * 8
    taps = conv_weight.reshape(LATENT, 9, channels).transpose(1, 0, 2)
    taps = jnp.concatenate([taps, taps], axis=1).reshape(72, channels)
    wide = jnp.concatenate(
        [embed_weight, embed_bias[None], jnp.zeros((7, width), F32)], axis=0
    )
    wslice = lax.dynamic_slice_in_dim(wide, me * part, part, axis=1)
    rows = wslice.shape[0]
    dma = pltpu.SemaphoreType.DMA
    chips = max(n // 2 - 1, 1)
    vm = pltpu.VMEM
    grad_features, conv, gb, emb = pl.pallas_call(
        functools.partial(kernel, images, height, across, n),
        out_shape=(
            jax.ShapeDtypeStruct((cells, channels), BF16),
            jax.ShapeDtypeStruct((72, channels), F32),
            jax.ShapeDtypeStruct((8, channels), F32),
            jax.ShapeDtypeStruct((inner, part), F32),
        ),
        in_specs=[pl.BlockSpec(memory_space=vm)] * 10,
        out_specs=[pl.BlockSpec(memory_space=vm)] * 4,
        scratch_shapes=[
            vm((2, pad_images, channels), F32),
            vm((n - 1, 2, pad_images, channels), F32),
            vm((cells, channels), F32),
            vm((cells, channels), F32),
            vm((cells, channels), BF16),
            vm((cells, channels), F32),
            vm((2, 8, cells), F32),
            vm((2, 8, cells), F32),
            vm((8, cells), F32),
            vm((2, 8, cells), F32),
            vm((rows, hidden), F32),
            vm((n - 1, rows, hidden), F32),
            vm((3 * inner, hidden), BF16),
            vm((n * share, align), BF16),
            vm((tokens, hidden), BF16),
            vm((tokens, hidden), F32),
            vm((tokens, hidden), BF16),
            vm((inner, hidden), F32),
            vm((n - 1, inner, hidden), F32),
            vm((2, pad_images, channels), F32),
            vm((n - 1, 2, pad_images, channels), F32),
            vm((4, pad_images, channels), F32),
            dma((n - 1,)), dma((n - 1,)), dma((n - 1,)), dma((n - 1,)),
            dma((chips,)), dma((chips,)), dma((chips + 1,)), dma((chips + 1,)),
            dma((2,)), dma((2,)), dma((2,)), dma((2,)),
            dma((n - 1,)), dma((n - 1,)), dma((n - 1,)), dma((n - 1,)),
        ],
        compiler_params=pltpu.CompilerParams(
            collective_id=0, has_side_effects=True, vmem_limit_bytes=60 * 1024 * 1024
        ),
        name="alignment_step",
    )(
        features.reshape(cells, channels), norm_gain[None], norm_bias[None], taps, wslice,
        proj_in, proj_in_bias[None], proj_out, proj_out_bias[None],
        targets.reshape(tokens, align),
    )
    embed_part = lax.dynamic_update_slice_in_dim(
        jnp.zeros((inner, width), F32), emb, me * part, axis=1
    )
    conv, gb, grad_embed = lax.psum((conv, gb, embed_part), ("rows", "batch"))
    grad_conv = (
        conv.reshape(9, 8, channels)[:, :LATENT].transpose(1, 0, 2).reshape(LATENT, 9 * channels)
    )
    return (
        grad_features.reshape(images, height, across, channels),
        grad_conv, gb[0], gb[1], grad_embed,
    )


def solution(mesh):
    in_specs = (
        P("batch", "rows", None, None), P(), P(), P(), P(), P(),
        P("rows", None), P(), P("rows", None), P(), P("batch", "rows", None, None),
    )
    out_specs = (P("batch", "rows", None, None), P(), P(), P(), P())
    return jax.shard_map(shards, mesh=mesh, in_specs=in_specs, out_specs=out_specs, check_vma=False)
```

```python
import functools

import jax
import jax.numpy as jnp
from jax import lax
from jax.experimental import pallas as pl
from jax.experimental.pallas import tpu as pltpu
from jax.sharding import PartitionSpec as P

GROUPS = 32
LATENT = 4
PATCH = 2
EPS_NORM = 1e-06
EPS_UNIT = 1e-06
F32 = jnp.float32
BF16 = jnp.bfloat16
NT = (((1,), (1,)), ((), ()))
TN = (((0,), (0,)), ((), ()))


def dot(a, b, dims=(((1,), (0,)), ((), ()))):
    return lax.dot_general(a, b, dims, preferred_element_type=F32)


def split(x, parts):
    out = []
    for _ in range(parts):
        part = x.astype(BF16).astype(F32)
        out.append(part)
        x = x - part
    return out


def exact_dot(x, exact, parts, dims=(((1,), (0,)), ((), ()))):
    rows = x.shape[0]
    full = dot(jnp.concatenate(split(x, parts), axis=0).astype(BF16), exact, dims)
    return sum(full[i * rows : (i + 1) * rows] for i in range(parts))


def kernel(
    images, height, across, n, nb,
    feat, gain, bias, taps, wslice, win, winb, wout, woutb, targ,
    out, conv_o, gain_o, bias_o, emb_o,
    st, st_in, nrm, slope, act, gs_ref, halo, halo_in, ghalo, ghalo_in,
    vpart, v_in, vcat, pout, hact, hslope, gh_ref, a_ref, a_in, fs, fs_in, stat,
    pack, pack_in, piece, piece_in, emb, emb_in, whole, whole_emb,
    s_send, s_recv, v_send, v_recv, x_send, x_recv, b_send, b_recv,
    h_send, h_recv, g_send, g_recv, a_send, a_recv, f_send, f_recv,
    p_send, p_recv, q_send, q_recv, e_send, e_recv, w_send, w_recv, y_send, y_recv,
):
    me = lax.axis_index("rows")
    cells, channels = feat.shape
    area = height * across
    per_group = channels // GROUPS
    members = n * area * per_group
    hidden = win.shape[1]
    share = wout.shape[0]
    tokens = targ.shape[0]
    tok_cols = across // PATCH
    prev, following = lax.rem(me + n - 1, n), lax.rem(me + 1, n)
    sibling = me + 1 - 2 * lax.rem(me, 2)

    def send(src, dst, ss, rs, peer):
        return pltpu.make_async_remote_copy(
            src_ref=src, dst_ref=dst, send_sem=ss, recv_sem=rs,
            device_id={"rows": peer}, device_id_type=pl.DeviceIdType.MESH,
        )

    def spread(src, dst, ss, rs):
        return [
            send(src, dst.at[k - 1], ss.at[k - 1], rs.at[k - 1], lax.rem(me + k, n))
            for k in range(1, n)
        ]

    barrier = pltpu.get_barrier_semaphore()
    for k in range(1, n):
        pl.semaphore_signal(
            barrier, inc=1, device_id={"rows": lax.rem(me + k, n)},
            device_id_type=pl.DeviceIdType.MESH,
        )
    group = lax.axis_index("batch")
    for k in range(1, nb):
        pl.semaphore_signal(
            barrier, inc=1, device_id={"batch": lax.rem(group + k, nb)},
            device_id_type=pl.DeviceIdType.MESH,
        )
    pl.semaphore_wait(barrier, n + nb - 2)

    def slab(owner):
        return pout.at[pl.ds(pl.multiple_of(owner * share, share), share), :]

    own = pl.ds(pl.multiple_of(me * share, share), share)
    cross = [
        send(wout, slab(me), x_send.at[k - 1], x_recv.at[k - 1], lax.rem(me + 2 * k, n))
        for k in range(1, n // 2)
    ]
    beside = [send(wout, slab(me), b_send.at[0], b_recv.at[0], sibling)]
    for copy in cross + beside:
        copy.start()
    pout[own, :] = wout[...]

    st[...] = jnp.zeros_like(st)

    def stats(b, carry):
        x = feat[pl.ds(pl.multiple_of(b * area, area), area), :].astype(F32)
        total = jnp.sum(x, axis=0, keepdims=True)
        centred = x - total / area
        st[0, pl.ds(b, 1), :] = total
        st[1, pl.ds(b, 1), :] = jnp.sum(centred * centred, axis=0, keepdims=True)
        return carry

    lax.fori_loop(0, images, stats, 0)
    stat_copies = spread(st, st_in, s_send, s_recv)
    for copy in stat_copies:
        copy.start()

    vpart[...] = exact_dot(wslice[...], win[...], 2)
    v_copies = spread(vpart, v_in, v_send, v_recv)
    for copy in v_copies:
        copy.start()
    same = (
        lax.broadcasted_iota(jnp.int32, (channels, channels), 0) // per_group
        == lax.broadcasted_iota(jnp.int32, (channels, channels), 1) // per_group
    )
    pool = jnp.where(same, 1.0, 0.0).astype(BF16)

    for copy in stat_copies:
        copy.wait()
    sums = [st[0]] + [st_in[k, 0] for k in range(n - 1)]
    squares = [st[1]] + [st_in[k, 1] for k in range(n - 1)]
    mean = exact_dot(sum(sums), pool, 3) / members
    spread_sq = sum(
        sq + area * jnp.square(total / area - mean) for total, sq in zip(sums, squares)
    )
    variance = exact_dot(spread_sq, pool, 3) / members
    stat[0] = mean
    stat[1] = lax.rsqrt(variance + EPS_NORM)

    def forward(b, carry):
        where = pl.ds(pl.multiple_of(b * area, area), area)
        x = feat[where, :].astype(F32)
        normed = (x - stat[0, pl.ds(b, 1), :]) * stat[1, pl.ds(b, 1), :]
        shifted = normed * gain[...] + bias[...]
        sig = jax.nn.sigmoid(shifted)
        nrm[where, :] = normed
        act[where, :] = (shifted * sig).astype(BF16)
        slope[where, :] = sig * (1.0 + shifted * (1.0 - sig))
        return carry

    lax.fori_loop(0, images, forward, 0)

    lane = lax.broadcasted_iota(jnp.int32, (8, cells), 1)
    col = lax.rem(lane, across)
    row = lax.rem(lane // across, height)

    def ahead(x, count):
        return pltpu.roll(x, (-count) % cells, 1) if count % cells else x

    def beside_col(x, off):
        if off == 0:
            return x
        ok = (col + off >= 0) & (col + off < across)
        return jnp.where(ok, ahead(x, off), 0.0)

    def above(x, arrived):
        edge = jnp.where(me > 0, ahead(arrived, (height - 1) * across), 0.0)
        return jnp.where(row == 0, edge, ahead(x, -across))

    def below(x, arrived):
        edge = jnp.where(me < n - 1, ahead(arrived, -(height - 1) * across), 0.0)
        return jnp.where(row == height - 1, edge, ahead(x, across))

    terms = dot(taps[...], act[...], NT)
    rows3 = []
    for dy in range(3):
        rows3.append(
            sum(
                beside_col(terms[(3 * dy + dx) * 8 : (3 * dy + dx + 1) * 8], dx - 1)
                for dx in range(3)
            )
        )
    halo[0] = rows3[0]
    halo[1] = rows3[2]
    halo_copies = [
        send(halo.at[0], halo_in.at[0], h_send.at[0], h_recv.at[0], following),
        send(halo.at[1], halo_in.at[1], h_send.at[1], h_recv.at[1], prev),
    ]
    for copy in halo_copies:
        copy.start()
    cell = lax.broadcasted_iota(jnp.int32, (cells, tokens), 0)
    tok = lax.broadcasted_iota(jnp.int32, (cells, tokens), 1)
    per_image = (height // PATCH) * tok_cols
    corner = (
        (tok // per_image) * area
        + (lax.rem(tok, per_image) // tok_cols) * (PATCH * across)
        + lax.rem(tok, tok_cols) * PATCH
    )
    away = cell - corner
    pick = [
        jnp.where(away == u * across + v, 1.0, 0.0).astype(BF16)
        for u in range(PATCH) for v in range(PATCH)
    ]
    for copy in v_copies:
        copy.wait()
    v_all = vpart[...] + sum(v_in[k] for k in range(n - 1))
    inner = PATCH * PATCH * LATENT
    v_hi, v_lo = split(v_all[0:inner], 2)
    vcat[...] = jnp.concatenate([v_hi, v_hi, v_lo], axis=0).astype(BF16)
    pre_bias = v_all[inner : inner + 1] + winb[...]
    for copy in halo_copies:
        copy.wait()
    latent = rows3[1] + above(rows3[0], halo_in[0]) + below(rows3[2], halo_in[1])
    first_half = lax.broadcasted_iota(jnp.int32, (8, tokens), 0) < LATENT
    blocks = []
    for u in range(PATCH):
        pair = [exact_dot(latent, pick[u * PATCH + v], 3) for v in range(PATCH)]
        blocks.append(jnp.where(first_half, pair[0], pair[1]))
    patches = jnp.concatenate(blocks, axis=0)
    p_hi, p_lo = split(patches, 2)
    pcat = jnp.concatenate([p_hi, p_lo, p_hi], axis=0).astype(BF16)

    for copy in cross:
        copy.wait()
    relay = []
    for k in range(1, n // 2):
        owner = lax.rem(me + n - 2 * k, n)
        relay.append(send(slab(owner), slab(owner), b_send.at[k], b_recv.at[k], sibling))
    for copy in relay:
        copy.start()

    step = hidden // 4
    for c in range(4):
        where = slice(c * step, (c + 1) * step)
        pre = dot(pcat, vcat[:, where], TN) + pre_bias[:, where]
        sig = jax.nn.sigmoid(pre)
        hact[:, where] = (pre * sig).astype(BF16)
        hslope[:, where] = sig * (1.0 + pre * (1.0 - sig))
    target = targ[...].astype(F32)
    unit_target = target * lax.rsqrt(jnp.sum(target * target, axis=1, keepdims=True) + EPS_UNIT)
    for copy in beside + relay:
        copy.wait()
    projected = dot(hact[...], pout[...]) + woutb[...]
    inv_len = lax.rsqrt(jnp.sum(projected * projected, axis=1, keepdims=True) + EPS_UNIT)
    unit_proj = projected * inv_len
    cosine = jnp.sum(unit_proj * unit_target, axis=1, keepdims=True)
    grad_out = (-inv_len * (unit_target - cosine * unit_proj)).astype(BF16)
    for c in range(4):
        where = slice(c * step, (c + 1) * step)
        back = dot(grad_out, pout[where, :], NT)
        gh_ref[:, where] = (back * hslope[:, where]).astype(BF16)
    two = dot(vcat[inner:, :], gh_ref[...], NT)
    grad_patch = (two[0:inner] + two[inner:]).astype(BF16)

    grid = []
    for v in range(PATCH):
        grid.append(
            sum(
                dot(grad_patch[u * 8 : (u + 1) * 8], pick[u * PATCH + v], NT)
                for u in range(PATCH)
            )
        )
    low_rows = lax.broadcasted_iota(jnp.int32, (8, cells), 0) < LATENT
    both = jnp.where(low_rows, grid[0], grid[1])
    grad_lat = both + pltpu.roll(both, LATENT, 0)
    grad_lat = jnp.where(low_rows, grad_lat, 0.0)
    ghalo[...] = grad_lat
    ghalo_copies = [
        send(ghalo, ghalo_in.at[0], g_send.at[0], g_recv.at[0], following),
        send(ghalo, ghalo_in.at[1], g_send.at[1], g_recv.at[1], prev),
    ]
    for copy in ghalo_copies:
        copy.start()
    wide = dot(pcat[0 : 2 * inner], gh_ref[...])
    a_ref[...] = wide[0:inner] + wide[inner:]
    a_copies = spread(a_ref, a_in, a_send, a_recv)
    for copy in a_copies:
        copy.start()
    for copy in ghalo_copies:
        copy.wait()
    by_row = [below(grad_lat, ghalo_in[1]), grad_lat, above(grad_lat, ghalo_in[0])]
    grad_taps = jnp.concatenate(
        [beside_col(by_row[dy], 1 - dx) for dy in range(3) for dx in range(3)], axis=0
    ).astype(BF16)
    gs_ref[...] = dot(grad_taps, taps[...], TN)
    fs[...] = jnp.zeros_like(fs)

    def backward(b, carry):
        where = pl.ds(pl.multiple_of(b * area, area), area)
        gs = gs_ref[where, :] * slope[where, :]
        gs_ref[where, :] = gs
        fs[0, pl.ds(b, 1), :] = jnp.sum(gs, axis=0, keepdims=True)
        fs[1, pl.ds(b, 1), :] = jnp.sum(gs * nrm[where, :], axis=0, keepdims=True)
        return carry

    lax.fori_loop(0, images, backward, 0)
    f_copies = spread(fs, fs_in, f_send, f_recv)
    for copy in f_copies:
        copy.start()
    conv = dot(grad_taps, act[...])
    gain_row = jnp.sum(fs[1], axis=0, keepdims=True)
    bias_row = jnp.sum(fs[0], axis=0, keepdims=True)
    row8 = lax.broadcasted_iota(jnp.int32, (8, channels), 0)
    per = pack.shape[1] // 8
    lanes = pack.shape[2]
    for i in range(5):
        block = conv[16 * i : 16 * i + 8]
        if i < 4:
            block = block + pltpu.roll(conv[16 * i + 8 : 16 * i + 16], LATENT, 0)
        else:
            block = jnp.where(row8 == LATENT, gain_row, block)
            block = jnp.where(row8 == LATENT + 1, bias_row, block)
        for c in range(channels // lanes):
            t = 5 * c + i
            pack[t // per, (t % per) * 8 : (t % per + 1) * 8, :] = (
                block[:, c * lanes : (c + 1) * lanes]
            )
    for t in range(5 * (channels // lanes), n * per):
        pack[t // per, (t % per) * 8 : (t % per + 1) * 8, :] = jnp.zeros((8, lanes), F32)
    p_copies = []
    for k in range(1, n):
        peer = lax.rem(me + k, n)
        p_copies.append(
            send(pack.at[peer], pack_in.at[k - 1], p_send.at[k - 1], p_recv.at[k - 1], peer)
        )
    for copy in p_copies:
        copy.start()
    for copy in a_copies:
        copy.wait()
    a_all = a_ref[...] + sum(a_in[k] for k in range(n - 1))
    emb[...] = exact_dot(a_all, win[...], 2, NT)

    def across_batch(src, dst, ss, rs):
        return [
            pltpu.make_async_remote_copy(
                src_ref=src, dst_ref=dst.at[k - 1], send_sem=ss.at[k - 1], recv_sem=rs.at[k - 1],
                device_id={"batch": lax.rem(group + k, nb)}, device_id_type=pl.DeviceIdType.MESH,
            )
            for k in range(1, nb)
        ]

    q_copies = across_batch(emb, emb_in, e_send, e_recv)
    for copy in q_copies:
        copy.start()
    for copy in p_copies:
        copy.wait()
    piece[...] = pack[me] + sum(pack_in[k] for k in range(n - 1))
    piece_copies = across_batch(piece, piece_in, q_send, q_recv)
    for copy in piece_copies:
        copy.start()
    for copy in f_copies:
        copy.wait()
    for i in range(2):
        total = (fs[i] + sum(fs_in[k, i] for k in range(n - 1))) * gain[...]
        stat_i = exact_dot(total, pool, 3) / members
        stat[2 + i] = stat_i

    def finish(b, carry):
        where = pl.ds(pl.multiple_of(b * area, area), area)
        one = pl.ds(b, 1)
        out[where, :] = (
            stat[1, one, :]
            * (gs_ref[where, :] * gain[...] - stat[2, one, :] - nrm[where, :] * stat[3, one, :])
        ).astype(BF16)
        return carry

    lax.fori_loop(0, images // 2, finish, 0)
    for copy in q_copies + piece_copies:
        copy.wait()
    whole[me] = ordered(piece, piece_in, group, nb)
    whole_emb[me] = ordered(emb, emb_in, group, nb)
    w_copies = []
    for k in range(1, n):
        peer = lax.rem(me + k, n)
        w_copies.append(send(whole.at[me], whole.at[me], w_send.at[k - 1], w_recv.at[k - 1], peer))
        w_copies.append(
            send(whole_emb.at[me], whole_emb.at[me], y_send.at[k - 1], y_recv.at[k - 1], peer)
        )
    for copy in w_copies:
        copy.start()
    lax.fori_loop(images // 2, images, finish, 0)
    for copy in w_copies:
        copy.wait()
    for c in range(channels // lanes):
        at = slice(c * lanes, (c + 1) * lanes)
        for i in range(5):
            t = 5 * c + i
            tile = whole[t // per, (t % per) * 8 : (t % per + 1) * 8, :]
            for half in range(2):
                tap = 2 * i + half
                rows = tile[half * LATENT : (half + 1) * LATENT]
                if tap < 9:
                    start = tap * channels + c * lanes
                    conv_o[:, start : start + lanes] = rows
                else:
                    gain_o[:, at] = rows[0:1]
                    bias_o[:, at] = rows[1:2]
    part = emb.shape[1]
    for k in range(n):
        emb_o[:, k * part : (k + 1) * part] = whole_emb[k]


def ordered(own, arrived, group, nb):
    total = None
    for g in range(nb):
        slot = lax.rem(group + nb - g, nb)
        value = arrived[jnp.maximum(slot - 1, 0)] if nb > 1 else own[...]
        value = jnp.where(slot == 0, own[...], value)
        total = value if total is None else total + value
    return total


def shards(
    features, norm_gain, norm_bias, conv_weight, embed_weight, embed_bias,
    proj_in, proj_in_bias, proj_out, proj_out_bias, targets,
):
    images, height, across, channels = features.shape
    n = lax.axis_size("rows")
    nb = lax.axis_size("batch")
    lanes = 128
    per = -(-(5 * (channels // lanes)) // n)
    me = lax.axis_index("rows")
    cells = images * height * across
    align = targets.shape[-1]
    tokens = targets.shape[0] * targets.shape[1] * targets.shape[2]
    inner, width = embed_weight.shape
    part, hidden = proj_in.shape
    share = proj_out.shape[0]
    pad_images = -(-images // 8) * 8
    taps = conv_weight.reshape(LATENT, 9, channels).transpose(1, 0, 2)
    taps = jnp.concatenate([taps, taps], axis=1).reshape(72, channels)
    wide = jnp.concatenate(
        [embed_weight, embed_bias[None], jnp.zeros((7, width), F32)], axis=0
    )
    wslice = lax.dynamic_slice_in_dim(wide, me * part, part, axis=1)
    rows = wslice.shape[0]
    dma = pltpu.SemaphoreType.DMA
    chips = max(n // 2 - 1, 1)
    vm = pltpu.VMEM
    grad_features, grad_conv, grad_gain, grad_bias, grad_embed = pl.pallas_call(
        functools.partial(kernel, images, height, across, n, nb),
        out_shape=(
            jax.ShapeDtypeStruct((cells, channels), BF16),
            jax.ShapeDtypeStruct((LATENT, 9 * channels), F32),
            jax.ShapeDtypeStruct((1, channels), F32),
            jax.ShapeDtypeStruct((1, channels), F32),
            jax.ShapeDtypeStruct((inner, width), F32),
        ),
        in_specs=[pl.BlockSpec(memory_space=vm)] * 10,
        out_specs=[pl.BlockSpec(memory_space=vm)] * 5,
        scratch_shapes=[
            vm((2, pad_images, channels), F32),
            vm((n - 1, 2, pad_images, channels), F32),
            vm((cells, channels), F32),
            vm((cells, channels), F32),
            vm((cells, channels), BF16),
            vm((cells, channels), F32),
            vm((2, 8, cells), F32),
            vm((2, 8, cells), F32),
            vm((8, cells), F32),
            vm((2, 8, cells), F32),
            vm((rows, hidden), F32),
            vm((n - 1, rows, hidden), F32),
            vm((3 * inner, hidden), BF16),
            vm((n * share, align), BF16),
            vm((tokens, hidden), BF16),
            vm((tokens, hidden), F32),
            vm((tokens, hidden), BF16),
            vm((inner, hidden), F32),
            vm((n - 1, inner, hidden), F32),
            vm((2, pad_images, channels), F32),
            vm((n - 1, 2, pad_images, channels), F32),
            vm((4, pad_images, channels), F32),
            vm((n, per * 8, lanes), F32),
            vm((n - 1, per * 8, lanes), F32),
            vm((per * 8, lanes), F32),
            vm((max(nb - 1, 1), per * 8, lanes), F32),
            vm((inner, part), F32),
            vm((max(nb - 1, 1), inner, part), F32),
            vm((n, per * 8, lanes), F32),
            vm((n, inner, part), F32),
            dma((n - 1,)), dma((n - 1,)), dma((n - 1,)), dma((n - 1,)),
            dma((chips,)), dma((chips,)), dma((chips + 1,)), dma((chips + 1,)),
            dma((2,)), dma((2,)), dma((2,)), dma((2,)),
            dma((n - 1,)), dma((n - 1,)), dma((n - 1,)), dma((n - 1,)),
            dma((n - 1,)), dma((n - 1,)),
            dma((max(nb - 1, 1),)), dma((max(nb - 1, 1),)),
            dma((max(nb - 1, 1),)), dma((max(nb - 1, 1),)),
            dma((n - 1,)), dma((n - 1,)), dma((n - 1,)), dma((n - 1,)),
        ],
        compiler_params=pltpu.CompilerParams(
            collective_id=0, has_side_effects=True, vmem_limit_bytes=60 * 1024 * 1024
        ),
        name="alignment_step",
    )(
        features.reshape(cells, channels), norm_gain[None], norm_bias[None], taps, wslice,
        proj_in, proj_in_bias[None], proj_out, proj_out_bias[None],
        targets.reshape(tokens, align),
    )
    return (
        grad_features.reshape(images, height, across, channels),
        grad_conv, grad_gain[0], grad_bias[0], grad_embed,
    )


def solution(mesh):
    in_specs = (
        P("batch", "rows", None, None), P(), P(), P(), P(), P(),
        P("rows", None), P(), P("rows", None), P(), P("batch", "rows", None, None),
    )
    out_specs = (P("batch", "rows", None, None), P(), P(), P(), P())
    return jax.shard_map(shards, mesh=mesh, in_specs=in_specs, out_specs=out_specs, check_vma=False)
```
